256 devices in a mesh: batch: 8 (over z), seq: 32 (over y, x, core).
Axes of the slice: x: 4, y: 4, z: 8, core: 2. Of those that a mesh axis runs over, the one named last changes fastest.
Arguments:
- hidden: bfloat16 [8, 16384, 4096], P('batch', 'seq'), may hold values from -6 to 6
- score_direction: bfloat16 [8, 16384, 4096], P('batch', 'seq'), may hold values from -6 to 6
- adapter_down: bfloat16 [4096, 256], replicated, may hold values from -0.09375 to 0.09375
- adapter_up: bfloat16 [4096, 256], replicated, may hold values from -0.09375 to 0.09375
- rewards: float32 [8, 16384], P('batch', 'seq'), may hold values from -0.3125 to 0.3125
- values: float32 [8, 16384], P('batch', 'seq'), may hold values from -120 to 120
- log_ratio: float32 [8, 16384], P('batch', 'seq'), may hold values from -4 to 4
- lengths: int32 [8], P('batch'), may hold values from 4096 to 16384
Outputs:
- returns: float32 [8, 16384], P('batch', 'seq')
- grad_down: float32 [4096, 256], P(('batch', 'seq'))
- grad_up: float32 [4096, 256], P(('batch', 'seq'))
The draws below stay inside these ranges and needn't reach their ends.
All inputs are finite; a program needn't handle non-finite values.
Results may differ from the reference program's by a relative error of at most 0.0029.
Values sent between devices are 32-bit elements; how exact they have to be, the bound alone decides.
A program may use at most 128 MiB of HBM per device.

```python
import math
import jax
import jax.numpy as jnp
from jax import lax

MODEL_DIM = 4096
ADAPTER_RANK = 256
SEQS = 8
LEN = 16384
N_SEQ = 32


def draw_values(key, part):
    base = jax.random.normal(jax.random.fold_in(key, 11), (SEQS, LEN), jnp.float32)
    base = jnp.clip(base, -6.0, 6.0)
    return base


def place_ends(result, own_key, smallest, top_value):
    longest = result.shape.index(max(result.shape))
    spots = []
    for shift in (0, 1):
        where = [jax.random.randint(jax.random.fold_in(own_key, axis), (), 0, length) for axis, length in enumerate(result.shape)]
        where[longest] = (where[longest] + shift) % result.shape[longest]
        spots.append(tuple(where))
    return result.at[spots[0]].set(smallest).at[spots[1]].set(top_value)


def level_of(own_key, extent, cuts, low, largest):
    level = 1.0
    for dim, parts in cuts:
        heights = jax.random.uniform(jax.random.fold_in(jax.random.fold_in(own_key, 6), dim), (parts,), jnp.float32, low / len(cuts), largest / len(cuts))
        level = level * jnp.repeat(jnp.exp(heights), extent[dim] // parts).reshape((-1,) + (1,) * (len(extent) - 1 - dim))
    return level


def noise(stream_key, shape, width, most, split=(), kind=jnp.bfloat16):
    level = level_of(stream_key, shape, split, -0.22, 0.18) if split else 1.0
    array = jax.random.normal(stream_key, shape, jnp.float32) * width * level
    return jnp.minimum(jnp.maximum(array, -most), most).astype(kind)


def setup_inputs(seed: int = 0) -> dict:
    key_of = jax.random.split(jax.random.key(seed), 9)
    hidden = noise(key_of[0], (SEQS, LEN, MODEL_DIM), 1.0, 6.0, ((0, 8), (1, 32)))
    score_direction = noise(key_of[1], (SEQS, LEN, MODEL_DIM), 1.0, 6.0, ((0, 8), (1, 32)))
    adapter_down = noise(key_of[2], (MODEL_DIM, ADAPTER_RANK), MODEL_DIM ** -0.5, 0.09375)
    adapter_up = noise(key_of[3], (MODEL_DIM, ADAPTER_RANK), MODEL_DIM ** -0.5, 0.09375)
    rewards = noise(key_of[4], (SEQS, LEN), 0.02, 0.3125, ((0, 8), (1, 32)), jnp.float32)
    values = draw_values(jax.random.fold_in(key_of[8], 71), 0)
    log_ratio = noise(key_of[6], (SEQS, LEN), 0.3, 4.0, ((0, 8), (1, 32)), jnp.float32)
    lengths = place_ends(jax.random.randint(key_of[7], (SEQS,), LEN // 4, LEN + 1), jax.random.fold_in(key_of[7], 1), LEN // 4, LEN).astype(jnp.int32)
    return {"hidden": hidden, "score_direction": score_direction, "adapter_down": adapter_down, "adapter_up": adapter_up, "rewards": rewards, "values": values, "log_ratio": log_ratio, "lengths": lengths}


ratio_cap = 2.0
weight_gain = 0.08

def reference(hidden, score_direction, adapter_down, adapter_up, rewards, values, log_ratio, lengths):
    seq_count, total_len, model_width = hidden.shape
    low_rank_product = adapter_down.shape[1]
    shard_len = total_len // N_SEQ
    positions = jnp.arange(total_len, dtype=jnp.int32)
    valid = (positions[None, :] < lengths[:, None]).astype(jnp.float32)
    live = (rewards * valid).reshape(seq_count, N_SEQ, shard_len)
    inner = jnp.arange(shard_len, dtype=jnp.int32)
    offsets = (inner[None, :] - inner[:, None]).astype(jnp.float32)
    discount_mat = jnp.where(offsets >= 0, jnp.exp(-offsets / total_len), jnp.zeros_like(offsets))
    within = jnp.einsum('sbk,tk->sbt', live, discount_mat, precision=lax.Precision.HIGHEST)
    firsts = within[:, :, 0]
    block_decay = jnp.exp(jnp.asarray(-shard_len / total_len, jnp.float32))

    def advance(incoming, first_now):
        return (first_now + block_decay * incoming, incoming)
    zeros_seq = jnp.zeros((seq_count,), jnp.float32)
    _, carried = lax.scan(advance, zeros_seq, jnp.transpose(firsts)[::-1])
    carried = jnp.transpose(carried[::-1])
    tail_decay = jnp.exp(-(shard_len - inner).astype(jnp.float32) / total_len)
    returns = (within + tail_decay[None, None, :] * carried[:, :, None]).reshape(seq_count, total_len)
    advantage = returns - values
    adapter_scale = 1.0 / math.sqrt(low_rank_product)
    seq_weight = weight_gain * math.sqrt(total_len * low_rank_product / seq_count) / lengths.astype(jnp.float32)

    def per_seq(totals, pieces):
        hidden_rows, direction_rows, adv_seq, gap_seq, valid_seq, weight_seq = pieces
        down_projected = jnp.dot(hidden_rows, adapter_down, preferred_element_type=jnp.float32)
        up_projected = jnp.dot(direction_rows, adapter_up, preferred_element_type=jnp.float32)
        weight_update = adapter_scale * lax.optimization_barrier(jnp.sum(down_projected * up_projected, axis=-1))
        importance = jnp.exp(gap_seq + weight_update)
        token_weights = valid_seq * jnp.minimum(importance, ratio_cap) * adv_seq * weight_seq
        up_scaled_map = (-adapter_scale * token_weights[:, None] * up_projected).astype(jnp.bfloat16)
        down_scaled_map = (-adapter_scale * token_weights[:, None] * down_projected).astype(jnp.bfloat16)
        dims = (((0,), (0,)), ((), ()))
        grad_a = lax.dot_general(hidden_rows, up_scaled_map, dims, preferred_element_type=jnp.float32)
        grad_b = lax.dot_general(direction_rows, down_scaled_map, dims, preferred_element_type=jnp.float32)
        return ((totals[0] + grad_a, totals[1] + grad_b), None)
    empty = jnp.zeros((model_width, low_rank_product), jnp.float32)
    (raw_down, raw_up), _ = lax.scan(per_seq, (empty, empty), (hidden, score_direction, advantage, log_ratio, valid, seq_weight))
    grad_norm = jnp.sqrt(jnp.sum(raw_down * raw_down) + jnp.sum(raw_up * raw_up))
    clip_norm = 0.5 * math.sqrt(2.0 * model_width * low_rank_product)
    factor = clip_norm / jnp.maximum(grad_norm, clip_norm)
    return (returns, raw_down * factor, raw_up * factor)
```

```python
import functools
import math

import jax
import jax.numpy as jnp
from jax import lax
from jax.experimental import pallas as pl
from jax.experimental.pallas import tpu as pltpu
from jax.sharding import PartitionSpec as P

ratio_cap = 2.0
weight_gain = 0.08

SIDE = 4
DEEP = 8
PLANE = 2 * SIDE * SIDE
TOKENS = 512
SLAB = 512
RANK = 256
CHUNKS = 2 * DEEP
LAG_JOIN, LAG_PASS, LAG_TURN, LAG_PASS2, LAG_DONE = 1, 2, 3, 4, 5
MESH = pl.DeviceIdType.MESH


def kernel(
    total_len,
    seq_total,
    hidden,
    direction,
    down_map,
    up_map,
    rewards,
    values,
    log_ratio,
    lengths,
    returns_out,
    down_out,
    up_out,
    acts,
    maps,
    proj,
    scaled,
    part,
    from_core,
    first,
    pass1,
    side1,
    second,
    pass2,
    side2,
    third,
    from_z,
    carry,
    norm_plane,
    norm_z,
    act_sem,
    map_sem,
    core_sem,
    pass1_sem,
    side1_sem,
    pass2_sem,
    side2_sem,
    small_sem,
    send_sem,
):
    z = lax.axis_index("batch")
    me = lax.axis_index("seq")
    core = me % 2
    x = (me // 2) % SIDE
    y = me // (2 * SIDE)
    f = core * y + (1 - core) * x
    s = core * x + (1 - core) * y

    def seq_of(f_at, s_at):
        y_at = core * f_at + (1 - core) * s_at
        x_at = core * s_at + (1 - core) * f_at
        return (y_at * SIDE + x_at) * 2 + core

    partner = me + 1 - 2 * core
    f_right, f_left = seq_of((f + 1) % SIDE, s), seq_of((f + SIDE - 1) % SIDE, s)
    s_right, s_left = seq_of(f, (s + 1) % SIDE), seq_of(f, (s + SIDE - 1) % SIDE)

    def load(g, k):
        src, table = (hidden, down_map) if g == 0 else (direction, up_map)
        columns = pl.ds(pl.multiple_of(k * SLAB, SLAB), SLAB)
        return (
            pltpu.make_async_copy(src.at[0, :, columns], acts.at[g, k], act_sem.at[g, k]),
            pltpu.make_async_copy(table.at[columns, :], maps.at[g, k], map_sem.at[g, k]),
        )

    for k in range(DEEP):
        for g in range(2):
            for copy in load(g, k):
                copy.start()

    barrier = pltpu.get_barrier_semaphore()

    @pl.loop(1, PLANE)
    def _(step):
        pl.semaphore_signal(
            barrier, inc=1, device_id=(z, (me + step) % PLANE), device_id_type=MESH
        )

    @pl.loop(1, DEEP)
    def _(step):
        pl.semaphore_signal(barrier, inc=1, device_id=((z + step) % DEEP, me), device_id_type=MESH)

    lane = lax.broadcasted_iota(jnp.int32, (8, TOKENS), 1)
    length = jnp.zeros((8, TOKENS), jnp.int32) + lengths[0]
    valid = (me * TOKENS + lane < length).astype(jnp.float32)
    within = jnp.broadcast_to(rewards[...], (8, TOKENS)) * valid
    span = 1
    while span < TOKENS:
        moved = pltpu.roll(within, TOKENS - span, 1)
        moved = jnp.where(lane < TOKENS - span, moved, 0.0)
        within = within + math.exp(-span / total_len) * moved
        span *= 2
    carry[me] = jnp.broadcast_to(within[0:1, 0:1], (1, 128))

    pl.semaphore_wait(barrier, PLANE - 1 + DEEP - 1)

    def to_plane(slots, sent, sem, step):
        return pltpu.make_async_remote_copy(
            src_ref=slots.at[me],
            dst_ref=slots.at[me],
            send_sem=send_sem.at[sent],
            recv_sem=small_sem.at[sem],
            device_id=(z, (me + step) % PLANE),
            device_id_type=MESH,
        )

    def to_column(slots, sent, sem, step):
        return pltpu.make_async_remote_copy(
            src_ref=slots.at[z],
            dst_ref=slots.at[z],
            send_sem=send_sem.at[sent],
            recv_sem=small_sem.at[sem],
            device_id=((z + step) % DEEP, me),
            device_id_type=MESH,
        )

    def wait_bytes(ref, sem):
        pltpu.make_async_copy(ref, ref, sem).wait()

    @pl.loop(1, PLANE)
    def _(step):
        to_plane(carry, 0, 0, step).start()

    for k in range(DEEP):
        for g in range(2):
            for copy in load(g, k):
                copy.wait()
            term = jnp.dot(acts[g, k], maps[g, k], preferred_element_type=jnp.float32)
            if k == 0:
                proj[g] = term
            else:
                proj[g] += term

    wait_bytes(carry.at[pl.ds(0, PLANE - 1)], small_sem.at[0])
    block = lax.broadcasted_iota(jnp.int32, (PLANE, 1, 128), 0)
    ahead = (block - me - 1).astype(jnp.float32)
    decay = jnp.exp(-ahead * TOKENS / total_len)
    carried = jnp.sum(jnp.where(block > me, decay * carry[...], 0.0), axis=0)
    carried = jnp.concatenate([carried] * (TOKENS // 128), axis=1)
    tail = jnp.exp(-(TOKENS - lane).astype(jnp.float32) / total_len)
    returns = within + tail * carried
    returns_out[...] = returns[0:1]
    gain = weight_gain * math.sqrt(total_len * RANK / seq_total) / length.astype(jnp.float32)
    base = valid * (returns - values[...]) * gain
    gap = jnp.broadcast_to(log_ratio[...], (8, TOKENS))
    scale = 1.0 / math.sqrt(RANK)
    here = lax.broadcasted_iota(jnp.int32, (128, 128), 0)
    diagonal = here == lax.broadcasted_iota(jnp.int32, (128, 128), 1)

    def upright(row):
        return jnp.sum(jnp.where(diagonal, row, 0.0), axis=1, keepdims=True)

    for b in range(TOKENS // 128):
        rows = slice(b * 128, b * 128 + 128)
        down, up = proj[0, rows], proj[1, rows]
        delta = scale * jnp.sum(down * up, axis=1, keepdims=True)
        weight = jnp.minimum(jnp.exp(upright(gap[0:1, rows]) + delta), ratio_cap)
        weight = -scale * (weight * upright(base[0:1, rows]))
        scaled[0, rows] = (weight * up).astype(jnp.bfloat16)
        scaled[1, rows] = (weight * down).astype(jnp.bfloat16)

    def plane_of(chunk):
        j = chunk // 2
        far = (DEEP - j) // 2
        return (z + DEEP + (2 * (j % 2) - 1) * far) % DEEP

    def core_copy(i):
        return pltpu.make_async_remote_copy(
            src_ref=part.at[i, :, :, 1 - core],
            dst_ref=from_core.at[i],
            send_sem=send_sem.at[1],
            recv_sem=core_sem.at[i],
            device_id=(z, partner),
            device_id_type=MESH,
        )

    def ring(blocks, passed, sides, pass_sems, side_sems, pass_send, side_send, at, right, left, half):
        low, high = pl.ds(0, half), pl.ds(half, half)
        after, before, across = (at + 1) % SIDE, (at + 3) % SIDE, (at + 2) % SIDE

        def copy(src, dst, send, recv, target):
            return pltpu.make_async_remote_copy(
                src_ref=src,
                dst_ref=dst,
                send_sem=send,
                recv_sem=recv,
                device_id=(z, target),
                device_id_type=MESH,
            )

        def begin(i):
            copy(blocks.at[i, across, low], passed.at[i, 0], pass_send, pass_sems.at[i], right).start()
            copy(blocks.at[i, across, high], passed.at[i, 1], pass_send, pass_sems.at[i], left).start()
            copy(blocks.at[i, after, high], sides.at[i, 0, high], side_send, side_sems.at[i], right).start()
            copy(blocks.at[i, before, low], sides.at[i, 1, low], side_send, side_sems.at[i], left).start()

        def forward(i):
            wait_bytes(passed.at[i], pass_sems.at[i])
            blocks[i, after, low] += passed[i, 0]
            copy(blocks.at[i, after, low], sides.at[i, 0, low], side_send, side_sems.at[i], right).start()
            blocks[i, before, high] += passed[i, 1]
            copy(blocks.at[i, before, high], sides.at[i, 1, high], side_send, side_sems.at[i], left).start()

        def finish(i):
            wait_bytes(sides.at[i], side_sems.at[i])
            return blocks[i, at] + sides[i, 0] + sides[i, 1]

        return begin, forward, finish

    begin1, forward1, finish1 = ring(
        first, pass1, side1, pass1_sem, side1_sem, send_sem.at[2], send_sem.at[3], f, f_right, f_left, 2
    )
    begin2, forward2, finish2 = ring(
        second, pass2, side2, pass2_sem, side2_sem, send_sem.at[4], send_sem.at[5], s, s_right, s_left, 1
    )

    @pl.loop(0, CHUNKS + LAG_DONE)
    def _(turn):
        @pl.when(turn < CHUNKS)
        def _():
            i = turn
            g = i % 2
            term = lax.dot_general(
                acts[g, plane_of(i)],
                scaled[g],
                (((0,), (0,)), ((), ())),
                preferred_element_type=jnp.float32,
            )
            part[i] = term.reshape(SIDE, SIDE, 2, 2, 8, RANK)
            core_copy(i).start()

        @pl.when((turn >= LAG_JOIN) & (turn < CHUNKS + LAG_JOIN))
        def _():
            i = turn - LAG_JOIN
            core_copy(i).wait_recv()

            @pl.loop(0, SIDE)
            def _(a):
                for b in range(SIDE):
                    y_at = core * a + (1 - core) * b
                    x_at = core * b + (1 - core) * a
                    first[i, a, b] = part[i, y_at, x_at, core] + from_core[i, y_at, x_at]

            begin1(i)

        @pl.when((turn >= LAG_PASS) & (turn < CHUNKS + LAG_PASS))
        def _():
            forward1(turn - LAG_PASS)

        @pl.when((turn >= LAG_TURN) & (turn < CHUNKS + LAG_TURN))
        def _():
            i = turn - LAG_TURN
            second[i] = finish1(i)
            begin2(i)

        @pl.when((turn >= LAG_PASS2) & (turn < CHUNKS + LAG_PASS2))
        def _():
            forward2(turn - LAG_PASS2)

        @pl.when(turn >= LAG_DONE)
        def _():
            i = turn - LAG_DONE

            @pl.when(i < CHUNKS - 2)
            def _():
                third[i] = finish2(i)
                pltpu.make_async_remote_copy(
                    src_ref=third.at[i],
                    dst_ref=from_z.at[z, i % 2],
                    send_sem=send_sem.at[6],
                    recv_sem=small_sem.at[1],
                    device_id=(plane_of(i), me),
                    device_id_type=MESH,
                ).start()

            @pl.when(i >= CHUNKS - 2)
            def _():
                from_z[z, i % 2] = finish2(i)

    wait_bytes(from_z.at[pl.ds(0, DEEP - 1)], small_sem.at[1])
    total = jnp.sum(from_z[...], axis=0)
    squares = total * total
    squares = squares[:, :, :, :128] + squares[:, :, :, 128:]
    squares = jnp.sum(squares.reshape(4, 8, 128), axis=0)
    norm_plane[me] = jnp.sum(squares, axis=0, keepdims=True)

    @pl.loop(1, PLANE)
    def _(step):
        to_plane(norm_plane, 7, 2, step).start()

    wait_bytes(norm_plane.at[pl.ds(0, PLANE - 1)], small_sem.at[2])
    norm_z[z] = jnp.sum(norm_plane[...], axis=0)

    @pl.loop(1, DEEP)
    def _(step):
        to_column(norm_z, 8, 3, step).start()

    wait_bytes(norm_z.at[pl.ds(0, DEEP - 1)], small_sem.at[3])
    grad_norm = jnp.sqrt(jnp.sum(jnp.sum(norm_z[...], axis=0), axis=1, keepdims=True))
    clip_norm = 0.5 * math.sqrt(2.0 * SLAB * DEEP * RANK)
    factor = clip_norm / jnp.maximum(grad_norm, clip_norm)
    down_out[...] = total[0].reshape(16, RANK) * factor
    up_out[...] = total[1].reshape(16, RANK) * factor

    wait_bytes(carry.at[pl.ds(0, PLANE - 1)], send_sem.at[0])
    wait_bytes(from_core, send_sem.at[1])
    wait_bytes(pass1, send_sem.at[2])
    wait_bytes(side1, send_sem.at[3])
    wait_bytes(pass2, send_sem.at[4])
    wait_bytes(side2, send_sem.at[5])
    wait_bytes(from_z.at[pl.ds(0, DEEP - 1)], send_sem.at[6])
    wait_bytes(norm_plane.at[pl.ds(0, PLANE - 1)], send_sem.at[7])
    wait_bytes(norm_z.at[pl.ds(0, DEEP - 1)], send_sem.at[8])


def local(hidden, direction, down_map, up_map, rewards, values, log_ratio, lengths):
    total_len = TOKENS * PLANE
    tile = (2, 8, RANK)
    f32 = jnp.float32
    dma = pltpu.SemaphoreType.DMA
    in_hbm = pl.BlockSpec(memory_space=pl.ANY)
    in_vmem = pl.BlockSpec(memory_space=pltpu.VMEM)
    return pl.pallas_call(
        functools.partial(kernel, total_len, DEEP),
        out_shape=(
            jax.ShapeDtypeStruct((1, TOKENS), f32),
            jax.ShapeDtypeStruct((16, RANK), f32),
            jax.ShapeDtypeStruct((16, RANK), f32),
        ),
        in_specs=[in_hbm] * 4 + [in_vmem] * 3 + [pl.BlockSpec(memory_space=pltpu.SMEM)],
        out_specs=(in_vmem, in_vmem, in_vmem),
        scratch_shapes=[
            pltpu.VMEM((2, DEEP, TOKENS, SLAB), jnp.bfloat16),
            pltpu.VMEM((2, DEEP, SLAB, RANK), jnp.bfloat16),
            pltpu.VMEM((2, TOKENS, RANK), f32),
            pltpu.VMEM((2, TOKENS, RANK), jnp.bfloat16),
            pltpu.VMEM((CHUNKS, SIDE, SIDE, 2, *tile), f32),
            pltpu.VMEM((CHUNKS, SIDE, SIDE, *tile), f32),
            pltpu.VMEM((CHUNKS, SIDE, SIDE, *tile), f32),
            pltpu.VMEM((CHUNKS, 2, SIDE // 2, *tile), f32),
            pltpu.VMEM((CHUNKS, 2, SIDE, *tile), f32),
            pltpu.VMEM((CHUNKS, SIDE, *tile), f32),
            pltpu.VMEM((CHUNKS, 2, 1, 8, RANK), f32),
            pltpu.VMEM((CHUNKS, 2, *tile), f32),
            pltpu.VMEM((CHUNKS, *tile), f32),
            pltpu.VMEM((DEEP, 2, *tile), f32),
            pltpu.VMEM((PLANE, 1, 128), f32),
            pltpu.VMEM((PLANE, 1, 128), f32),
            pltpu.VMEM((DEEP, 1, 128), f32),
            dma((2, DEEP)),
            dma((2, DEEP)),
            dma((CHUNKS,)),
            dma((CHUNKS,)),
            dma((CHUNKS,)),
            dma((CHUNKS,)),
            dma((CHUNKS,)),
            dma((4,)),
            dma((9,)),
        ],
        compiler_params=pltpu.CompilerParams(
            collective_id=0, has_side_effects=True, vmem_limit_bytes=60 * 1024 * 1024
        ),
    )(hidden, direction, down_map, up_map, rewards, values, log_ratio, lengths)


def solution(mesh):
    placed = (
        P("batch", "seq", None),
        P("batch", "seq", None),
        P(),
        P(),
        P("batch", "seq"),
        P("batch", "seq"),
        P("batch", "seq"),
        P("batch"),
    )
    return jax.shard_map(
        local,
        mesh=mesh,
        in_specs=placed,
        out_specs=(P("batch", "seq"), P(("batch", "seq"), None), P(("batch", "seq"), None)),
        check_vma=False,
    )
```

```python
import functools
import math

import jax
import jax.numpy as jnp
from jax import lax
from jax.experimental import pallas as pl
from jax.experimental.pallas import tpu as pltpu
from jax.sharding import PartitionSpec as P

ratio_cap = 2.0
weight_gain = 0.08

SIDE = 4
DEEP = 8
PLANE = 2 * SIDE * SIDE
TOKENS = 512
SLAB = 512
RANK = 256
HALF = SIDE // 2
STRAIGHT = 2
RINGED = DEEP - STRAIGHT
MESH = pl.DeviceIdType.MESH


def kernel(
    total_len,
    seq_total,
    hidden,
    direction,
    down_map,
    up_map,
    rewards_in,
    values_in,
    log_ratio_in,
    lengths_in,
    returns_out,
    total_out,
    factor_out,
    rewards,
    values,
    log_ratio,
    lengths,
    row_sem,
    acts,
    maps,
    proj,
    scaled,
    part,
    from_core,
    first_a,
    pass1_a,
    side1_a,
    second_a,
    in2_a,
    third_a,
    first_b,
    pass1_b,
    side1_b,
    second_b,
    in2_b,
    third_b,
    first_d,
    in1_d,
    second_d,
    in2_d,
    third_d,
    column,
    column_in,
    column_last,
    second_c,
    from_z,
    from_plane,
    carry,
    norm_plane,
    norm_z,
    act_sem,
    map_sem,
    core_sem,
    ring_sem,
    straight_sem,
    column_sem,
    small_sem,
    send_sem,
):
    z = lax.axis_index("batch")
    me = lax.axis_index("seq")
    core = me % 2
    x = (me // 2) % SIDE
    y = me // (2 * SIDE)
    f = core * y + (1 - core) * x
    s = core * x + (1 - core) * y

    def seq_of(f_at, s_at):
        y_at = core * f_at + (1 - core) * s_at
        x_at = core * s_at + (1 - core) * f_at
        return (y_at * SIDE + x_at) * 2 + core

    partner = me + 1 - 2 * core
    f_right, f_left = seq_of((f + 1) % SIDE, s), seq_of((f + SIDE - 1) % SIDE, s)
    s_right, s_left = seq_of(f, (s + 1) % SIDE), seq_of(f, (s + SIDE - 1) % SIDE)

    def load(g, k):
        src, table = (hidden, down_map) if g == 0 else (direction, up_map)
        columns = pl.ds(pl.multiple_of(k * SLAB, SLAB), SLAB)
        return (
            pltpu.make_async_copy(src.at[0, :, columns], acts.at[g, k], act_sem.at[g, k]),
            pltpu.make_async_copy(table.at[columns, :], maps.at[g, k], map_sem.at[g, k]),
        )

    barrier = pltpu.get_barrier_semaphore()

    @pl.loop(1, PLANE)
    def _(step):
        pl.semaphore_signal(
            barrier, inc=1, device_id=(z, (me + step) % PLANE), device_id_type=MESH
        )

    @pl.loop(1, DEEP)
    def _(step):
        pl.semaphore_signal(barrier, inc=1, device_id=((z + step) % DEEP, me), device_id_type=MESH)

    rows = (
        pltpu.make_async_copy(rewards_in, rewards, row_sem.at[0]),
        pltpu.make_async_copy(lengths_in, lengths, row_sem.at[1]),
        pltpu.make_async_copy(values_in, values, row_sem.at[2]),
        pltpu.make_async_copy(log_ratio_in, log_ratio, row_sem.at[3]),
    )
    for copy in rows:
        copy.start()

    for k in range(DEEP):
        for g in range(2):
            for copy in load(g, k):
                copy.start()

    for copy in rows:
        copy.wait()

    lane = lax.broadcasted_iota(jnp.int32, (8, TOKENS), 1)
    length = jnp.zeros((8, TOKENS), jnp.int32) + lengths[0]
    valid = (me * TOKENS + lane < length).astype(jnp.float32)
    within = jnp.broadcast_to(rewards[...], (8, TOKENS)) * valid
    span = 1
    while span < TOKENS:
        moved = pltpu.roll(within, TOKENS - span, 1)
        moved = jnp.where(lane < TOKENS - span, moved, 0.0)
        within = within + math.exp(-span / total_len) * moved
        span *= 2
    carry[me] = jnp.broadcast_to(within[0:1, 0:1], (1, 128))

    pl.semaphore_wait(barrier, PLANE - 1 + DEEP - 1)

    def to_plane(slots, sent, sem, step):
        return pltpu.make_async_remote_copy(
            src_ref=slots.at[me],
            dst_ref=slots.at[me],
            send_sem=send_sem.at[sent],
            recv_sem=small_sem.at[sem],
            device_id=(z, (me + step) % PLANE),
            device_id_type=MESH,
        )

    def to_column(slots, sent, sem, step):
        return pltpu.make_async_remote_copy(
            src_ref=slots.at[z],
            dst_ref=slots.at[z],
            send_sem=send_sem.at[sent],
            recv_sem=small_sem.at[sem],
            device_id=((z + step) % DEEP, me),
            device_id_type=MESH,
        )

    def wait_bytes(ref, sem):
        pltpu.make_async_copy(ref, ref, sem).wait()

    @pl.loop(1, PLANE)
    def _(step):
        to_plane(carry, 0, 0, step).start()

    for k in range(DEEP):
        for g in range(2):
            for copy in load(g, k):
                copy.wait()
            term = jnp.dot(acts[g, k], maps[g, k], preferred_element_type=jnp.float32)
            if k == 0:
                proj[g] = term
            else:
                proj[g] += term

    wait_bytes(carry.at[pl.ds(0, PLANE - 1)], small_sem.at[0])
    block = lax.broadcasted_iota(jnp.int32, (PLANE, 1, 128), 0)
    ahead = (block - me - 1).astype(jnp.float32)
    decay = jnp.exp(-ahead * TOKENS / total_len)
    carried = jnp.sum(jnp.where(block > me, decay * carry[...], 0.0), axis=0)
    carried = jnp.concatenate([carried] * (TOKENS // 128), axis=1)
    tail = jnp.exp(-(TOKENS - lane).astype(jnp.float32) / total_len)
    returns = within + tail * carried
    returns_out[...] = returns[0:1]
    gain = weight_gain * math.sqrt(total_len * RANK / seq_total) / length.astype(jnp.float32)
    base = valid * (returns - values[...]) * gain
    gap = jnp.broadcast_to(log_ratio[...], (8, TOKENS))
    scale = 1.0 / math.sqrt(RANK)
    here = lax.broadcasted_iota(jnp.int32, (128, 128), 0)
    diagonal = here == lax.broadcasted_iota(jnp.int32, (128, 128), 1)

    def upright(row):
        return jnp.sum(jnp.where(diagonal, row, 0.0), axis=1, keepdims=True)

    for b in range(TOKENS // 128):
        rows = slice(b * 128, b * 128 + 128)
        down, up = proj[0, rows], proj[1, rows]
        delta = scale * jnp.sum(down * up, axis=1, keepdims=True)
        weight = jnp.minimum(jnp.exp(upright(gap[0:1, rows]) + delta), ratio_cap)
        weight = -scale * (weight * upright(base[0:1, rows]))
        scaled[0, rows] = (weight * up).astype(jnp.bfloat16)
        scaled[1, rows] = (weight * down).astype(jnp.bfloat16)

    def plane_of(i):
        far = (DEEP - i) // 2
        return (z + DEEP + (2 * (i % 2) - 1) * far) % DEEP

    def send(src, dst, sent, received, target):
        pltpu.make_async_remote_copy(
            src_ref=src,
            dst_ref=dst,
            send_sem=send_sem.at[sent],
            recv_sem=received,
            device_id=target,
            device_id_type=MESH,
        ).start()

    def gradient(i, g, at):
        term = lax.dot_general(
            acts[g, plane_of(i)],
            scaled[g],
            (((0,), (0,)), ((), ())),
            preferred_element_type=jnp.float32,
        )
        part[at] = term.reshape(SIDE, SIDE, 2, 2, 8, RANK)
        send(part.at[at, :, :, 1 - core], from_core.at[at], 1, core_sem.at[at], (z, partner))

    def joined(at, a, b):
        y_at = core * a + (1 - core) * b
        x_at = core * b + (1 - core) * a
        return part[at, y_at, x_at, core] + from_core[at, y_at, x_at]

    def ring(blocks, passed, sides, row, at, right, left, low, high):
        after, before, across = (at + 1) % SIDE, (at + 3) % SIDE, (at + 2) % SIDE
        right, left = (z, right), (z, left)
        sent1, sent2 = 9 + 2 * row, 10 + 2 * row

        def begin(i):
            got, kept = ring_sem.at[row, 0, i], ring_sem.at[row, 1, i]
            send(blocks.at[(i, across, *low)], passed.at[i, 0], sent1, got, right)
            send(blocks.at[(i, across, *high)], passed.at[i, 1], sent1, got, left)
            send(blocks.at[(i, after, *high)], sides.at[(i, 0, *high)], sent2, kept, right)
            send(blocks.at[(i, before, *low)], sides.at[(i, 1, *low)], sent2, kept, left)

        def forward(i):
            got, kept = ring_sem.at[row, 0, i], ring_sem.at[row, 1, i]
            wait_bytes(passed.at[i], got)
            blocks[(i, after, *low)] += passed[i, 0]
            send(blocks.at[(i, after, *low)], sides.at[(i, 0, *low)], sent2, kept, right)
            blocks[(i, before, *high)] += passed[i, 1]
            send(blocks.at[(i, before, *high)], sides.at[(i, 1, *high)], sent2, kept, left)

        def finish(i):
            wait_bytes(sides.at[i], ring_sem.at[row, 1, i])
            return blocks[i, at] + sides[i, 0] + sides[i, 1]

        return begin, forward, finish

    def straight(blocks, arrived, row, at, target):
        def begin(i):
            for k in (2, 1, 3):
                other = (at + k) % SIDE
                send(
                    blocks.at[i, other],
                    arrived.at[i, k - 1],
                    13 + row,
                    straight_sem.at[row, i],
                    (z, target(other)),
                )

        def finish(i):
            wait_bytes(arrived.at[i], straight_sem.at[row, i])
            return blocks[i, at] + arrived[i, 0] + arrived[i, 1] + arrived[i, 2]

        return begin, finish

    def on_f(other):
        return seq_of(other, s)

    def on_s(other):
        return seq_of(f, other)

    halves = (pl.ds(0, HALF),), (pl.ds(HALF, HALF),)
    begin1_a, forward1_a, finish1_a = ring(first_a, pass1_a, side1_a, 0, f, f_right, f_left, *halves)
    begin1_b, forward1_b, finish1_b = ring(first_b, pass1_b, side1_b, 1, f, f_right, f_left, *halves)
    begin2_a, finish2_a = straight(second_a, in2_a, 0, s, on_s)
    begin2_b, finish2_b = straight(second_b, in2_b, 1, s, on_s)
    begin1_d, finish1_d = straight(first_d, in1_d, 2, f, on_f)
    begin2_d, finish2_d = straight(second_d, in2_d, 3, s, on_s)

    def product_a(i):
        gradient(i, 1, i)

    def join_a(i):
        wait_bytes(from_core.at[i], core_sem.at[i])

        @pl.loop(0, SIDE)
        def _(a):
            for b in range(SIDE):
                block = joined(i, a, b)
                column[b, plane_of(i), a] = block[0]
                first_a[i, a, b, 0] = block[1]

        begin1_a(i)

    def turn_a(i):
        second_a[i] = finish1_a(i)
        begin2_a(i)

    def done_a(i):
        @pl.when(i < DEEP - 1)
        def _():
            third_a[i] = finish2_a(i)
            send(third_a.at[i], from_z.at[z, pl.ds(0, 1)], 6, small_sem.at[1], (plane_of(i), me))

        @pl.when(i == DEEP - 1)
        def _():
            from_z[z, 0:1] = finish2_a(i)

    def product_b(i):
        gradient(i, 0, DEEP + i)

    def join_b(i):
        wait_bytes(from_core.at[DEEP + i], core_sem.at[DEEP + i])

        @pl.loop(0, SIDE)
        def _(a):
            for b in range(SIDE):
                first_b[i, a, b] = joined(DEEP + i, a, b)

        begin1_b(i)

    def turn_b(i):
        second_b[i] = finish1_b(i)
        begin2_b(i)

    def done_b(i):
        third_b[i] = finish2_b(i)
        send(third_b.at[i], from_z.at[z, pl.ds(1, 2)], 6, small_sem.at[1], (plane_of(i), me))

    def join_d(i):
        at = DEEP + RINGED + i
        wait_bytes(from_core.at[at], core_sem.at[at])

        @pl.loop(0, SIDE)
        def _(a):
            for b in range(SIDE):
                first_d[i, a, b] = joined(at, a, b)

        begin1_d(i)

    def turn_d(i):
        second_d[i] = finish1_d(i)
        begin2_d(i)

    def done_d(i):
        @pl.when(i < STRAIGHT - 1)
        def _():
            third_d[i] = finish2_d(i)
            send(third_d.at[i], from_z.at[z, pl.ds(1, 2)], 6, small_sem.at[1], (plane_of(RINGED + i), me))

        @pl.when(i == STRAIGHT - 1)
        def _():
            from_z[z, 1:3] = finish2_d(i)

    low, high = pl.ds(0, HALF), pl.ds(HALF, HALF)
    z_right, z_left = ((z + 1) % DEEP, me), ((z + DEEP - 1) % DEEP, me)

    def s_of(u):
        return (s + SIDE - 1 - u) % SIDE

    def plane(step):
        return (z + DEEP + step) % DEEP

    def begin_c(u):
        own, got = s_of(u), column_sem.at[u, 0]
        send(column.at[own, plane(4), low], column_in.at[u, 0, 0, 0], 4, got, z_right)
        send(column.at[own, plane(4), high], column_in.at[u, 0, 1, 0], 4, got, z_left)
        send(column.at[own, plane(3), high], column_in.at[u, 0, 0, 1], 4, got, z_right)
        send(column.at[own, plane(-3), low], column_in.at[u, 0, 1, 1], 4, got, z_left)

    def step_c(step):
        def run(u):
            own, got = s_of(u), column_sem.at[u, step]
            wait_bytes(column_in.at[u, step - 1], column_sem.at[u, step - 1])
            column[own, plane(4 - step), low] += column_in[u, step - 1, 0, 0]
            column[own, plane(step - 4), high] += column_in[u, step - 1, 1, 0]
            if step < 3:
                send(column.at[own, plane(4 - step), low], column_in.at[u, step, 0, 0], 4, got, z_right)
                send(column.at[own, plane(step - 4), high], column_in.at[u, step, 1, 0], 4, got, z_left)
                column[own, plane(3 - step), high] += column_in[u, step - 1, 0, 1]
                column[own, plane(step - 3), low] += column_in[u, step - 1, 1, 1]
                send(column.at[own, plane(3 - step), high], column_in.at[u, step, 0, 1], 4, got, z_right)
                send(column.at[own, plane(step - 3), low], column_in.at[u, step, 1, 1], 4, got, z_left)
            else:
                send(column.at[own, plane(1), low], column_last.at[u, 0], 5, got, z_right)
                send(column.at[own, plane(-1), high], column_last.at[u, 1], 5, got, z_left)

        return run

    def turn_c(u):
        own = s_of(u)
        wait_bytes(column_last.at[u], column_sem.at[u, 3])
        second_c[u, low] = column[own, z, low] + column_last[u, 0] + column_in[u, 2, 1, 1]
        second_c[u, high] = column[own, z, high] + column_last[u, 1] + column_in[u, 2, 0, 1]
        for k in range(SIDE):
            other = (f + k) % SIDE

            def share():
                send(
                    second_c.at[u, other],
                    from_plane.at[k * SIDE + SIDE - 1 - u],
                    3,
                    small_sem.at[4],
                    (z, seq_of(other, own)),
                )

            if k == 0:
                pl.when(u < SIDE - 1)(share)
            else:
                share()

        @pl.when(u == SIDE - 1)
        def _():
            from_plane[0] = second_c[u, f]

    schedule = (
        (0, 1, DEEP, product_a),
        (8, 1, DEEP, product_b),
        (2, 1, DEEP, join_a),
        (10, 1, SIDE, begin_c),
        (10, 1, RINGED, join_b),
        (16, 1, STRAIGHT, join_d),
        (15, 1, SIDE, step_c(1)),
        (20, 1, SIDE, step_c(2)),
        (25, 1, SIDE, step_c(3)),
        (30, 1, SIDE, turn_c),
        (8, 1, DEEP, forward1_a),
        (18, 1, RINGED, forward1_b),
        (14, 1, DEEP, turn_a),
        (26, 1, RINGED, turn_b),
        (21, 1, DEEP, done_a),
        (34, 1, RINGED, done_b),
        (30, 1, STRAIGHT, turn_d),
        (40, 1, STRAIGHT, done_d),
    )

    @pl.loop(0, max(start + every * (count - 1) for start, every, count, _ in schedule) + 1)
    def _(turn):
        for start, every, count, stage in schedule:
            now = (turn >= start) & (turn < start + every * count)
            if every > 1:
                now = now & ((turn - start) % every == 0)
            pl.when(now)(functools.partial(stage, (turn - start) // every))

    wait_bytes(from_z.at[pl.ds(0, DEEP - 1)], small_sem.at[1])
    wait_bytes(from_plane.at[pl.ds(1, SIDE * SIDE - 1)], small_sem.at[4])
    summed = jnp.sum(from_z[...], axis=0)
    total = jnp.concatenate([summed[1:3], jnp.sum(from_plane[...], axis=0)[None], summed[0:1]], axis=0)
    squares = total * total
    squares = jnp.sum(squares[:, :, :128] + squares[:, :, 128:], axis=0)
    norm_plane[me] = jnp.sum(squares, axis=0, keepdims=True)

    @pl.loop(1, PLANE)
    def _(step):
        to_plane(norm_plane, 7, 2, step).start()

    wait_bytes(norm_plane.at[pl.ds(0, PLANE - 1)], small_sem.at[2])
    norm_z[z] = jnp.sum(norm_plane[...], axis=0)

    @pl.loop(1, DEEP)
    def _(step):
        to_column(norm_z, 8, 3, step).start()

    wait_bytes(norm_z.at[pl.ds(0, DEEP - 1)], small_sem.at[3])
    grad_norm = jnp.sqrt(jnp.sum(jnp.sum(norm_z[...], axis=0), axis=1, keepdims=True))
    clip_norm = 0.5 * math.sqrt(2.0 * SLAB * DEEP * RANK)
    factor = clip_norm / jnp.maximum(grad_norm, clip_norm)
    total_out[...] = total.reshape(2, 16, RANK)
    factor_out[...] = jnp.broadcast_to(factor, (1, 128))

    sends = (
        (0, carry.at[pl.ds(0, PLANE - 1)]),
        (1, from_core),
        (3, from_plane.at[pl.ds(1, SIDE * SIDE - 1)]),
        (4, column_in),
        (5, column_last),
        (6, from_z.at[pl.ds(0, DEEP - 1)]),
        (7, norm_plane.at[pl.ds(0, PLANE - 1)]),
        (8, norm_z.at[pl.ds(0, DEEP - 1)]),
        (9, pass1_a),
        (10, side1_a),
        (11, pass1_b),
        (12, side1_b),
        (13, in2_a),
        (14, in2_b),
        (15, in1_d),
        (16, in2_d),
    )
    for sent, ref in sends:
        wait_bytes(ref, send_sem.at[sent])


def clip(returns, total, factor, returns_out, down_out, up_out):
    returns_out[...] = returns[...]
    down_out[...] = total[0] * factor[0:1, 0:1]
    up_out[...] = total[1] * factor[0:1, 0:1]


def local(hidden, direction, down_map, up_map, rewards, values, log_ratio, lengths):
    total_len = TOKENS * PLANE
    tile = (8, RANK)
    f32 = jnp.float32
    dma = pltpu.SemaphoreType.DMA

    def ring_buffers(chunks, tiles):
        block = (tiles, *tile)
        return (
            pltpu.VMEM((chunks, SIDE, SIDE, *block), f32),
            pltpu.VMEM((chunks, 2, HALF, *block), f32),
            pltpu.VMEM((chunks, 2, SIDE, *block), f32),
            pltpu.VMEM((chunks, SIDE, *block), f32),
            pltpu.VMEM((chunks, SIDE - 1, *block), f32),
            pltpu.VMEM((chunks, *block), f32),
        )

    in_hbm = pl.BlockSpec(memory_space=pl.ANY)
    in_vmem = pl.BlockSpec(memory_space=pltpu.VMEM)
    returns, total, factor = pl.pallas_call(
        functools.partial(kernel, total_len, DEEP),
        out_shape=(
            jax.ShapeDtypeStruct((1, TOKENS), f32),
            jax.ShapeDtypeStruct((2, 16, RANK), f32),
            jax.ShapeDtypeStruct((1, 128), f32),
        ),
        in_specs=[in_hbm] * 8,
        out_specs=(in_vmem, in_vmem, in_vmem),
        scratch_shapes=[
            pltpu.VMEM((1, TOKENS), f32),
            pltpu.VMEM((1, TOKENS), f32),
            pltpu.VMEM((1, TOKENS), f32),
            pltpu.SMEM((1,), jnp.int32),
            dma((4,)),
            pltpu.VMEM((2, DEEP, TOKENS, SLAB), jnp.bfloat16),
            pltpu.VMEM((2, DEEP, SLAB, RANK), jnp.bfloat16),
            pltpu.VMEM((2, TOKENS, RANK), f32),
            pltpu.VMEM((2, TOKENS, RANK), jnp.bfloat16),
            pltpu.VMEM((2 * DEEP, SIDE, SIDE, 2, 2, *tile), f32),
            pltpu.VMEM((2 * DEEP, SIDE, SIDE, 2, *tile), f32),
            *ring_buffers(DEEP, 1),
            *ring_buffers(RINGED, 2),
            pltpu.VMEM((STRAIGHT, SIDE, SIDE, 2, *tile), f32),
            pltpu.VMEM((STRAIGHT, SIDE - 1, SIDE, 2, *tile), f32),
            pltpu.VMEM((STRAIGHT, SIDE, 2, *tile), f32),
            pltpu.VMEM((STRAIGHT, SIDE - 1, 2, *tile), f32),
            pltpu.VMEM((STRAIGHT, 2, *tile), f32),
            pltpu.VMEM((SIDE, DEEP, SIDE, *tile), f32),
            pltpu.VMEM((SIDE, 3, 2, 2, HALF, *tile), f32),
            pltpu.VMEM((SIDE, 2, HALF, *tile), f32),
            pltpu.VMEM((SIDE, SIDE, *tile), f32),
            pltpu.VMEM((DEEP, 3, *tile), f32),
            pltpu.VMEM((SIDE * SIDE, *tile), f32),
            pltpu.VMEM((PLANE, 1, 128), f32),
            pltpu.VMEM((PLANE, 1, 128), f32),
            pltpu.VMEM((DEEP, 1, 128), f32),
            dma((2, DEEP)),
            dma((2, DEEP)),
            dma((2 * DEEP,)),
            dma((2, 2, DEEP)),
            dma((4, DEEP)),
            dma((SIDE, 4)),
            dma((5,)),
            dma((17,)),
        ],
        compiler_params=pltpu.CompilerParams(
            collective_id=0, has_side_effects=True, vmem_limit_bytes=60 * 1024 * 1024
        ),
    )(hidden, direction, down_map, up_map, rewards, values, log_ratio, lengths)
    return pl.pallas_call(
        clip,
        out_shape=(
            jax.ShapeDtypeStruct((1, TOKENS), f32),
            jax.ShapeDtypeStruct((16, RANK), f32),
            jax.ShapeDtypeStruct((16, RANK), f32),
        ),
        in_specs=[in_vmem] * 3,
        out_specs=(in_vmem, in_vmem, in_vmem),
    )(returns, total, factor)


def solution(mesh):
    placed = (
        P("batch", "seq", None),
        P("batch", "seq", None),
        P(),
        P(),
        P("batch", "seq"),
        P("batch", "seq"),
        P("batch", "seq"),
        P("batch"),
    )
    return jax.shard_map(
        local,
        mesh=mesh,
        in_specs=placed,
        out_specs=(P("batch", "seq"), P(("batch", "seq"), None), P(("batch", "seq"), None)),
        check_vma=False,
    )
```

```python
import functools
import math

import jax
import jax.numpy as jnp
from jax import lax
from jax.experimental import pallas as pl
from jax.experimental.pallas import tpu as pltpu
from jax.sharding import PartitionSpec as P

ratio_cap = 2.0
weight_gain = 0.08

SIDE = 4
DEEP = 8
PLANE = 2 * SIDE * SIDE
TOKENS = 512
SLAB = 512
RANK = 256
HALF = SIDE // 2
STRAIGHT = 2
RINGED = DEEP - STRAIGHT
MESH = pl.DeviceIdType.MESH


def kernel(
    total_len,
    seq_total,
    hidden,
    direction,
    down_map,
    up_map,
    rewards_in,
    values_in,
    log_ratio_in,
    lengths_in,
    returns_out,
    total_out,
    factor_out,
    rewards,
    values,
    log_ratio,
    lengths,
    row_sem,
    acts,
    maps,
    proj,
    scaled,
    part,
    from_core,
    first_a,
    pass1_a,
    side1_a,
    second_a,
    in2_a,
    third_a,
    first_b,
    pass1_b,
    side1_b,
    second_b,
    in2_b,
    third_b,
    first_d,
    in1_d,
    second_d,
    in2_d,
    third_d,
    column,
    column_in,
    column_last,
    second_c,
    from_z,
    from_plane,
    carry,
    norm_plane,
    norm_z,
    act_sem,
    map_sem,
    core_sem,
    ring_sem,
    straight_sem,
    column_sem,
    small_sem,
    send_sem,
):
    z = lax.axis_index("batch")
    me = lax.axis_index("seq")
    core = me % 2
    x = (me // 2) % SIDE
    y = me // (2 * SIDE)
    f = core * y + (1 - core) * x
    s = core * x + (1 - core) * y

    def seq_of(f_at, s_at):
        y_at = core * f_at + (1 - core) * s_at
        x_at = core * s_at + (1 - core) * f_at
        return (y_at * SIDE + x_at) * 2 + core

    partner = me + 1 - 2 * core
    f_right, f_left = seq_of((f + 1) % SIDE, s), seq_of((f + SIDE - 1) % SIDE, s)
    s_right, s_left = seq_of(f, (s + 1) % SIDE), seq_of(f, (s + SIDE - 1) % SIDE)

    def load(g, k):
        src, table = (hidden, down_map) if g == 0 else (direction, up_map)
        columns = pl.ds(pl.multiple_of(k * SLAB, SLAB), SLAB)
        return (
            pltpu.make_async_copy(src.at[0, :, columns], acts.at[g, k], act_sem.at[g, k]),
            pltpu.make_async_copy(table.at[columns, :], maps.at[g, k], map_sem.at[g, k]),
        )

    barrier = pltpu.get_barrier_semaphore()

    @pl.loop(1, PLANE)
    def _(step):
        pl.semaphore_signal(
            barrier, inc=1, device_id=(z, (me + step) % PLANE), device_id_type=MESH
        )

    @pl.loop(1, DEEP)
    def _(step):
        pl.semaphore_signal(barrier, inc=1, device_id=((z + step) % DEEP, me), device_id_type=MESH)

    rows = (
        pltpu.make_async_copy(rewards_in, rewards, row_sem.at[0]),
        pltpu.make_async_copy(lengths_in, lengths, row_sem.at[1]),
        pltpu.make_async_copy(values_in, values, row_sem.at[2]),
        pltpu.make_async_copy(log_ratio_in, log_ratio, row_sem.at[3]),
    )
    for copy in rows:
        copy.start()

    for k in range(DEEP):
        for g in range(2):
            for copy in load(g, k):
                copy.start()

    for copy in rows:
        copy.wait()

    lane = lax.broadcasted_iota(jnp.int32, (8, TOKENS), 1)
    length = jnp.zeros((8, TOKENS), jnp.int32) + lengths[0]
    valid = (me * TOKENS + lane < length).astype(jnp.float32)
    within = jnp.broadcast_to(rewards[...], (8, TOKENS)) * valid
    span = 1
    while span < TOKENS:
        moved = pltpu.roll(within, TOKENS - span, 1)
        moved = jnp.where(lane < TOKENS - span, moved, 0.0)
        within = within + math.exp(-span / total_len) * moved
        span *= 2
    carry[me] = jnp.broadcast_to(within[0:1, 0:1], (1, 128))

    pl.semaphore_wait(barrier, PLANE - 1 + DEEP - 1)

    def to_plane(slots, sent, sem, step):
        return pltpu.make_async_remote_copy(
            src_ref=slots.at[me],
            dst_ref=slots.at[me],
            send_sem=send_sem.at[sent],
            recv_sem=small_sem.at[sem],
            device_id=(z, (me + step) % PLANE),
            device_id_type=MESH,
        )

    def to_column(slots, sent, sem, step):
        return pltpu.make_async_remote_copy(
            src_ref=slots.at[z],
            dst_ref=slots.at[z],
            send_sem=send_sem.at[sent],
            recv_sem=small_sem.at[sem],
            device_id=((z + step) % DEEP, me),
            device_id_type=MESH,
        )

    def wait_bytes(ref, sem):
        pltpu.make_async_copy(ref, ref, sem).wait()

    @pl.loop(1, PLANE)
    def _(step):
        to_plane(carry, 0, 0, step).start()

    for k in range(DEEP):
        for g in range(2):
            for copy in load(g, k):
                copy.wait()
            term = jnp.dot(acts[g, k], maps[g, k], preferred_element_type=jnp.float32)
            if k == 0:
                proj[g] = term
            else:
                proj[g] += term

    wait_bytes(carry.at[pl.ds(0, PLANE - 1)], small_sem.at[0])
    block = lax.broadcasted_iota(jnp.int32, (PLANE, 1, 128), 0)
    ahead = (block - me - 1).astype(jnp.float32)
    decay = jnp.exp(-ahead * TOKENS / total_len)
    carried = jnp.sum(jnp.where(block > me, decay * carry[...], 0.0), axis=0)
    carried = jnp.concatenate([carried] * (TOKENS // 128), axis=1)
    tail = jnp.exp(-(TOKENS - lane).astype(jnp.float32) / total_len)
    returns = within + tail * carried
    returns_out[...] = returns[0:1]
    gain = weight_gain * math.sqrt(total_len * RANK / seq_total) / length.astype(jnp.float32)
    base = valid * (returns - values[...]) * gain
    gap = jnp.broadcast_to(log_ratio[...], (8, TOKENS))
    scale = 1.0 / math.sqrt(RANK)
    here = lax.broadcasted_iota(jnp.int32, (128, 128), 0)
    diagonal = here == lax.broadcasted_iota(jnp.int32, (128, 128), 1)

    def upright(row):
        return jnp.sum(jnp.where(diagonal, row, 0.0), axis=1, keepdims=True)

    for b in range(TOKENS // 128):
        rows = slice(b * 128, b * 128 + 128)
        down, up = proj[0, rows], proj[1, rows]
        delta = scale * jnp.sum(down * up, axis=1, keepdims=True)
        weight = jnp.minimum(jnp.exp(upright(gap[0:1, rows]) + delta), ratio_cap)
        weight = -scale * (weight * upright(base[0:1, rows]))
        scaled[0, rows] = (weight * up).astype(jnp.bfloat16)
        scaled[1, rows] = (weight * down).astype(jnp.bfloat16)

    def plane_of(i):
        far = (DEEP - i) // 2
        return (z + DEEP + (2 * (i % 2) - 1) * far) % DEEP

    def send(src, dst, sent, received, target):
        pltpu.make_async_remote_copy(
            src_ref=src,
            dst_ref=dst,
            send_sem=send_sem.at[sent],
            recv_sem=received,
            device_id=target,
            device_id_type=MESH,
        ).start()

    def gradient(i, g, at):
        term = lax.dot_general(
            acts[g, plane_of(i)],
            scaled[g],
            (((0,), (0,)), ((), ())),
            preferred_element_type=jnp.float32,
        )
        part[at] = term.reshape(SIDE, SIDE, 2, 2, 8, RANK)
        send(part.at[at, :, :, 1 - core], from_core.at[at], 1, core_sem.at[at], (z, partner))

    def joined(at, a, b):
        y_at = core * a + (1 - core) * b
        x_at = core * b + (1 - core) * a
        return part[at, y_at, x_at, core] + from_core[at, y_at, x_at]

    def ring(blocks, passed, sides, row, at, right, left, low, high):
        after, before, across = (at + 1) % SIDE, (at + 3) % SIDE, (at + 2) % SIDE
        right, left = (z, right), (z, left)
        sent1, sent2 = 9 + 2 * row, 10 + 2 * row

        def begin(i):
            got, kept = ring_sem.at[row, 0, i], ring_sem.at[row, 1, i]
            send(blocks.at[(i, across, *low)], passed.at[i, 0], sent1, got, right)
            send(blocks.at[(i, across, *high)], passed.at[i, 1], sent1, got, left)
            send(blocks.at[(i, after, *high)], sides.at[(i, 0, *high)], sent2, kept, right)
            send(blocks.at[(i, before, *low)], sides.at[(i, 1, *low)], sent2, kept, left)

        def forward(i):
            got, kept = ring_sem.at[row, 0, i], ring_sem.at[row, 1, i]
            wait_bytes(passed.at[i], got)
            blocks[(i, after, *low)] += passed[i, 0]
            send(blocks.at[(i, after, *low)], sides.at[(i, 0, *low)], sent2, kept, right)
            blocks[(i, before, *high)] += passed[i, 1]
            send(blocks.at[(i, before, *high)], sides.at[(i, 1, *high)], sent2, kept, left)

        def finish(i):
            wait_bytes(sides.at[i], ring_sem.at[row, 1, i])
            return blocks[i, at] + sides[i, 0] + sides[i, 1]

        return begin, forward, finish

    def straight(blocks, arrived, row, at, target):
        def begin(i):
            for k in (2, 1, 3):
                other = (at + k) % SIDE
                send(
                    blocks.at[i, other],
                    arrived.at[i, k - 1],
                    13 + row,
                    straight_sem.at[row, i],
                    (z, target(other)),
                )

        def finish(i):
            wait_bytes(arrived.at[i], straight_sem.at[row, i])
            return blocks[i, at] + arrived[i, 0] + arrived[i, 1] + arrived[i, 2]

        return begin, finish

    def on_f(other):
        return seq_of(other, s)

    def on_s(other):
        return seq_of(f, other)

    halves = (pl.ds(0, HALF),), (pl.ds(HALF, HALF),)
    begin1_a, forward1_a, finish1_a = ring(first_a, pass1_a, side1_a, 0, f, f_right, f_left, *halves)
    begin1_b, forward1_b, finish1_b = ring(first_b, pass1_b, side1_b, 1, f, f_right, f_left, *halves)
    begin2_a, finish2_a = straight(second_a, in2_a, 0, s, on_s)
    begin2_b, finish2_b = straight(second_b, in2_b, 1, s, on_s)
    begin1_d, finish1_d = straight(first_d, in1_d, 2, f, on_f)
    begin2_d, finish2_d = straight(second_d, in2_d, 3, s, on_s)

    def product_a(i):
        gradient(i, 1, i)

    def join_a(i):
        wait_bytes(from_core.at[i], core_sem.at[i])

        @pl.loop(0, SIDE)
        def _(a):
            for b in range(SIDE):
                block = joined(i, a, b)
                column[b, plane_of(i), a] = block[0]
                first_a[i, a, b, 0] = block[1]

        begin1_a(i)

    def turn_a(i):
        second_a[i] = finish1_a(i)
        begin2_a(i)

    def done_a(i):
        @pl.when(i < DEEP - 1)
        def _():
            third_a[i] = finish2_a(i)
            send(third_a.at[i], from_z.at[z, pl.ds(0, 1)], 6, small_sem.at[1], (plane_of(i), me))

        @pl.when(i == DEEP - 1)
        def _():
            from_z[z, 0:1] = finish2_a(i)

    def product_b(i):
        gradient(i, 0, DEEP + i)

    def join_b(i):
        wait_bytes(from_core.at[DEEP + i], core_sem.at[DEEP + i])

        @pl.loop(0, SIDE)
        def _(a):
            for b in range(SIDE):
                first_b[i, a, b] = joined(DEEP + i, a, b)

        begin1_b(i)

    def turn_b(i):
        second_b[i] = finish1_b(i)
        begin2_b(i)

    def done_b(i):
        third_b[i] = finish2_b(i)
        send(third_b.at[i], from_z.at[z, pl.ds(1, 2)], 6, small_sem.at[1], (plane_of(i), me))

    def join_d(i):
        at = DEEP + RINGED + i
        wait_bytes(from_core.at[at], core_sem.at[at])

        @pl.loop(0, SIDE)
        def _(a):
            for b in range(SIDE):
                first_d[i, a, b] = joined(at, a, b)

        begin1_d(i)

    def turn_d(i):
        second_d[i] = finish1_d(i)
        begin2_d(i)

    def done_d(i):
        @pl.when(i < STRAIGHT - 1)
        def _():
            third_d[i] = finish2_d(i)
            send(third_d.at[i], from_z.at[z, pl.ds(1, 2)], 6, small_sem.at[1], (plane_of(RINGED + i), me))

        @pl.when(i == STRAIGHT - 1)
        def _():
            from_z[z, 1:3] = finish2_d(i)

    low, high = pl.ds(0, HALF), pl.ds(HALF, HALF)
    z_right, z_left = ((z + 1) % DEEP, me), ((z + DEEP - 1) % DEEP, me)

    def s_of(u):
        return (s + SIDE - 1 - u) % SIDE

    def plane(step):
        return (z + DEEP + step) % DEEP

    def begin_c(u):
        own, got = s_of(u), column_sem.at[u, 0]
        send(column.at[own, plane(4), low], column_in.at[u, 0, 0, 0], 4, got, z_right)
        send(column.at[own, plane(4), high], column_in.at[u, 0, 1, 0], 4, got, z_left)
        send(column.at[own, plane(3), high], column_in.at[u, 0, 0, 1], 4, got, z_right)
        send(column.at[own, plane(-3), low], column_in.at[u, 0, 1, 1], 4, got, z_left)

    def step_c(step):
        def run(u):
            own, got = s_of(u), column_sem.at[u, step]
            wait_bytes(column_in.at[u, step - 1], column_sem.at[u, step - 1])
            column[own, plane(4 - step), low] += column_in[u, step - 1, 0, 0]
            column[own, plane(step - 4), high] += column_in[u, step - 1, 1, 0]
            if step < 3:
                send(column.at[own, plane(4 - step), low], column_in.at[u, step, 0, 0], 4, got, z_right)
                send(column.at[own, plane(step - 4), high], column_in.at[u, step, 1, 0], 4, got, z_left)
                column[own, plane(3 - step), high] += column_in[u, step - 1, 0, 1]
                column[own, plane(step - 3), low] += column_in[u, step - 1, 1, 1]
                send(column.at[own, plane(3 - step), high], column_in.at[u, step, 0, 1], 4, got, z_right)
                send(column.at[own, plane(step - 3), low], column_in.at[u, step, 1, 1], 4, got, z_left)
            else:
                send(column.at[own, plane(1), low], column_last.at[u, 0], 5, got, z_right)
                send(column.at[own, plane(-1), high], column_last.at[u, 1], 5, got, z_left)

        return run

    def turn_c(u):
        own = s_of(u)
        wait_bytes(column_last.at[u], column_sem.at[u, 3])
        second_c[u, low] = column[own, z, low] + column_last[u, 0] + column_in[u, 2, 1, 1]
        second_c[u, high] = column[own, z, high] + column_last[u, 1] + column_in[u, 2, 0, 1]
        for k in range(SIDE):
            other = (f + k) % SIDE

            def share():
                send(
                    second_c.at[u, other],
                    from_plane.at[k * SIDE + SIDE - 1 - u],
                    3,
                    small_sem.at[4],
                    (z, seq_of(other, own)),
                )

            if k == 0:
                pl.when(u < SIDE - 1)(share)
            else:
                share()

        @pl.when(u == SIDE - 1)
        def _():
            from_plane[0] = second_c[u, f]

    schedule = (
        (0, 1, DEEP, product_a),
        (8, 1, DEEP, product_b),
        (2, 1, DEEP, join_a),
        (10, 1, SIDE, begin_c),
        (10, 1, RINGED, join_b),
        (16, 1, STRAIGHT, join_d),
        (16, 1, SIDE, step_c(1)),
        (22, 1, SIDE, step_c(2)),
        (28, 1, SIDE, step_c(3)),
        (33, 1, SIDE, turn_c),
        (8, 1, DEEP, forward1_a),
        (17, 1, RINGED, forward1_b),
        (14, 1, DEEP, turn_a),
        (25, 1, RINGED, turn_b),
        (21, 1, DEEP, done_a),
        (33, 1, RINGED, done_b),
        (31, 1, STRAIGHT, turn_d),
        (41, 1, STRAIGHT, done_d),
    )

    @pl.loop(0, max(start + every * (count - 1) for start, every, count, _ in schedule) + 1)
    def _(turn):
        for start, every, count, stage in schedule:
            now = (turn >= start) & (turn < start + every * count)
            if every > 1:
                now = now & ((turn - start) % every == 0)
            pl.when(now)(functools.partial(stage, (turn - start) // every))

    wait_bytes(from_z.at[pl.ds(0, DEEP - 1)], small_sem.at[1])
    wait_bytes(from_plane.at[pl.ds(1, SIDE * SIDE - 1)], small_sem.at[4])
    summed = jnp.sum(from_z[...], axis=0)
    total = jnp.concatenate([summed[1:3], jnp.sum(from_plane[...], axis=0)[None], summed[0:1]], axis=0)
    squares = total * total
    squares = jnp.sum(squares[:, :, :128] + squares[:, :, 128:], axis=0)
    norm_plane[me] = jnp.sum(squares, axis=0, keepdims=True)

    @pl.loop(1, PLANE)
    def _(step):
        to_plane(norm_plane, 7, 2, step).start()

    wait_bytes(norm_plane.at[pl.ds(0, PLANE - 1)], small_sem.at[2])
    norm_z[z] = jnp.sum(norm_plane[...], axis=0)

    @pl.loop(1, DEEP)
    def _(step):
        to_column(norm_z, 8, 3, step).start()

    wait_bytes(norm_z.at[pl.ds(0, DEEP - 1)], small_sem.at[3])
    grad_norm = jnp.sqrt(jnp.sum(jnp.sum(norm_z[...], axis=0), axis=1, keepdims=True))
    clip_norm = 0.5 * math.sqrt(2.0 * SLAB * DEEP * RANK)
    factor = clip_norm / jnp.maximum(grad_norm, clip_norm)
    total_out[...] = total.reshape(2, 16, RANK)
    factor_out[...] = jnp.broadcast_to(factor, (1, 128))

    sends = (
        (0, carry.at[pl.ds(0, PLANE - 1)]),
        (1, from_core),
        (3, from_plane.at[pl.ds(1, SIDE * SIDE - 1)]),
        (4, column_in),
        (5, column_last),
        (6, from_z.at[pl.ds(0, DEEP - 1)]),
        (7, norm_plane.at[pl.ds(0, PLANE - 1)]),
        (8, norm_z.at[pl.ds(0, DEEP - 1)]),
        (9, pass1_a),
        (10, side1_a),
        (11, pass1_b),
        (12, side1_b),
        (13, in2_a),
        (14, in2_b),
        (15, in1_d),
        (16, in2_d),
    )
    for sent, ref in sends:
        wait_bytes(ref, send_sem.at[sent])


def clip(returns, total, factor, returns_out, down_out, up_out):
    returns_out[...] = returns[...]
    down_out[...] = total[0] * factor[0:1, 0:1]
    up_out[...] = total[1] * factor[0:1, 0:1]


def local(hidden, direction, down_map, up_map, rewards, values, log_ratio, lengths):
    total_len = TOKENS * PLANE
    tile = (8, RANK)
    f32 = jnp.float32
    dma = pltpu.SemaphoreType.DMA

    def ring_buffers(chunks, tiles):
        block = (tiles, *tile)
        return (
            pltpu.VMEM((chunks, SIDE, SIDE, *block), f32),
            pltpu.VMEM((chunks, 2, HALF, *block), f32),
            pltpu.VMEM((chunks, 2, SIDE, *block), f32),
            pltpu.VMEM((chunks, SIDE, *block), f32),
            pltpu.VMEM((chunks, SIDE - 1, *block), f32),
            pltpu.VMEM((chunks, *block), f32),
        )

    in_hbm = pl.BlockSpec(memory_space=pl.ANY)
    in_vmem = pl.BlockSpec(memory_space=pltpu.VMEM)
    returns, total, factor = pl.pallas_call(
        functools.partial(kernel, total_len, DEEP),
        out_shape=(
            jax.ShapeDtypeStruct((1, TOKENS), f32),
            jax.ShapeDtypeStruct((2, 16, RANK), f32),
            jax.ShapeDtypeStruct((1, 128), f32),
        ),
        in_specs=[in_hbm] * 8,
        out_specs=(in_vmem, in_vmem, in_vmem),
        scratch_shapes=[
            pltpu.VMEM((1, TOKENS), f32),
            pltpu.VMEM((1, TOKENS), f32),
            pltpu.VMEM((1, TOKENS), f32),
            pltpu.SMEM((1,), jnp.int32),
            dma((4,)),
            pltpu.VMEM((2, DEEP, TOKENS, SLAB), jnp.bfloat16),
            pltpu.VMEM((2, DEEP, SLAB, RANK), jnp.bfloat16),
            pltpu.VMEM((2, TOKENS, RANK), f32),
            pltpu.VMEM((2, TOKENS, RANK), jnp.bfloat16),
            pltpu.VMEM((2 * DEEP, SIDE, SIDE, 2, 2, *tile), f32),
            pltpu.VMEM((2 * DEEP, SIDE, SIDE, 2, *tile), f32),
            *ring_buffers(DEEP, 1),
            *ring_buffers(RINGED, 2),
            pltpu.VMEM((STRAIGHT, SIDE, SIDE, 2, *tile), f32),
            pltpu.VMEM((STRAIGHT, SIDE - 1, SIDE, 2, *tile), f32),
            pltpu.VMEM((STRAIGHT, SIDE, 2, *tile), f32),
            pltpu.VMEM((STRAIGHT, SIDE - 1, 2, *tile), f32),
            pltpu.VMEM((STRAIGHT, 2, *tile), f32),
            pltpu.VMEM((SIDE, DEEP, SIDE, *tile), f32),
            pltpu.VMEM((SIDE, 3, 2, 2, HALF, *tile), f32),
            pltpu.VMEM((SIDE, 2, HALF, *tile), f32),
            pltpu.VMEM((SIDE, SIDE, *tile), f32),
            pltpu.VMEM((DEEP, 3, *tile), f32),
            pltpu.VMEM((SIDE * SIDE, *tile), f32),
            pltpu.VMEM((PLANE, 1, 128), f32),
            pltpu.VMEM((PLANE, 1, 128), f32),
            pltpu.VMEM((DEEP, 1, 128), f32),
            dma((2, DEEP)),
            dma((2, DEEP)),
            dma((2 * DEEP,)),
            dma((2, 2, DEEP)),
            dma((4, DEEP)),
            dma((SIDE, 4)),
            dma((5,)),
            dma((17,)),
        ],
        compiler_params=pltpu.CompilerParams(
            collective_id=0, has_side_effects=True, vmem_limit_bytes=60 * 1024 * 1024
        ),
    )(hidden, direction, down_map, up_map, rewards, values, log_ratio, lengths)
    return pl.pallas_call(
        clip,
        out_shape=(
            jax.ShapeDtypeStruct((1, TOKENS), f32),
            jax.ShapeDtypeStruct((16, RANK), f32),
            jax.ShapeDtypeStruct((16, RANK), f32),
        ),
        in_specs=[in_vmem] * 3,
        out_specs=(in_vmem, in_vmem, in_vmem),
    )(returns, total, factor)


def solution(mesh):
    placed = (
        P("batch", "seq", None),
        P("batch", "seq", None),
        P(),
        P(),
        P("batch", "seq"),
        P("batch", "seq"),
        P("batch", "seq"),
        P("batch"),
    )
    return jax.shard_map(
        local,
        mesh=mesh,
        in_specs=placed,
        out_specs=(P("batch", "seq"), P(("batch", "seq"), None), P(("batch", "seq"), None)),
        check_vma=False,
    )
```
